32 devices in a mesh: lat: 4 (over y, core), lon: 8 (over z, x).
Axes of the slice: x: 2, y: 2, z: 4, core: 2. Of those that a mesh axis runs over, the one named last changes fastest.
Arguments:
- coarse: bfloat16 [30720, 1104], P(('lat', 'lon')), may hold values from -6 to 6
- w_mix: bfloat16 [69, 64], replicated, may hold values from -0.75 to 0.75
- interp: bfloat16 [16, 256], replicated, may hold values from -1.5 to 1.5
- kernel: bfloat16 [3, 3, 64, 64], replicated, may hold values from -0.25 to 0.25
- bias: float32 [64], replicated, may hold values from -3 to 3
- block_ids: int32 [32, 144], replicated, may hold values from 0 to 30719, as said below
- valid: int32 [32, 144], replicated, may hold values from 0 to 1, as said below
Outputs:
- fine_out: bfloat16 [64, 1152, 1024], P(None, 'lat', 'lon')
The draws below stay inside these ranges and needn't reach their ends.
Inputs may be any that keep to these rules, and one draw needn't show every extreme that they name: `block_ids`: the coarse grid has 96 block rows and 320 block columns, held block-cyclically: block (r, c) is row ((r mod 4) * 8 + c mod 8) * 960 + (r div 4) * 40 + c div 8 of coarse. Slot p of tile t holds block (r0 + (t div 8) * 18 + p div 8, (c0 + (t mod 8) * 8 + p mod 8) mod (320)), with offsets r0 and c0 common to all tiles. Among the valid slots of one tile at most 5 name blocks of one device, and in every tile exactly 5 valid slots name blocks of some one device. Every tile has 5 or more valid slots.
All inputs are finite; a program needn't handle non-finite values.
Results may differ from the reference program's by a relative error of at most 0.0055.
Values may be sent and summed in bfloat16 or wider, within the bound.
A program may use at most 192 MiB of HBM per device.

```python
import jax
import jax.numpy as jnp
from jax import lax

C_IN = 69
C = 64
CB_ROWS = 24
CB_COLS = 40
PR = 18
PC = 8
CB_DEV = 960
PATCHES = 144
TH = 288
TW = 128
TILES = 32
BLOCKS = 30720
N_LAT = 4
N_LON = 8
DEVICES = 32


def route_table(key):
    base = jax.random.fold_in(key, 11)
    keys = jax.random.split(base, 6)
    grid_cols = N_LON * CB_COLS
    row_start = jax.random.randint(keys[0], (), 0, N_LAT * (CB_ROWS - PR) + 1)
    col_start = jax.random.randint(keys[1], (), 0, grid_cols)
    tiles = jnp.arange(DEVICES, dtype=jnp.int32)
    tile_lat = tiles // N_LON
    tile_lon = tiles % N_LON
    slots = jnp.arange(PATCHES, dtype=jnp.int32)
    patch_row = slots // PC
    patch_col = slots % PC
    rows = row_start + tile_lat[:, None] * PR + patch_row[None, :]
    cols = (col_start + tile_lon[:, None] * PC + patch_col[None, :]) % grid_cols
    owner = rows % N_LAT * N_LON + cols % N_LON
    local = rows // N_LAT * CB_COLS + cols // N_LON
    ids = (owner * CB_DEV + local).astype(jnp.int32)
    slope_row = jax.random.randint(keys[2], (DEVICES, 1), -3, 4)
    slope_col = jax.random.randint(keys[3], (DEVICES, 1), -3, 4)
    rough = jax.random.randint(keys[4], (DEVICES, PATCHES), 0, 4)
    cut = jax.random.randint(keys[5], (DEVICES, 1), -2 * PC, PC // 2 + 1)
    score = slope_row * (patch_row[None, :] - PR // 2) + slope_col * (patch_col[None, :] - PC // 2) + rough
    forced = owner == owner[:, :1]
    live = ((score >= cut) | forced).astype(jnp.int32)
    return (ids, live)


def draw_block_ids(key, part):
    return route_table(key)[0]


def draw_valid(key, part):
    return route_table(key)[1]


def shard_levels(own_key, shape, shards, least, largest):
    def one(position, shards_of):
        heights = jax.random.uniform(jax.random.fold_in(jax.random.fold_in(own_key, 6), position), (shards_of,), jnp.float32, least / len(shards), largest / len(shards))
        return jnp.repeat(jnp.exp(heights), shape[position] // shards_of).reshape((-1,) + (1,) * (len(shape) - position - 1))

    loudness = one(*shards[0])
    for cut in shards[1:]:
        loudness = loudness * one(*cut)
    return loudness


def gaussian(stream_key, extent, scale, bound, cuts=(), kind=jnp.bfloat16):
    entries = jax.random.normal(stream_key, extent, jnp.float32) * scale
    if len(cuts) > 0:
        entries = shard_levels(stream_key, extent, cuts, -0.22, 0.18) * entries
    return jnp.clip(entries, min=-bound, max=bound).astype(kind)


def setup_inputs(seed: int = 0) -> dict:
    arg_keys = jax.random.split(jax.random.key(seed), 8)
    return {
        "coarse": gaussian(arg_keys[0], (BLOCKS, 16 * C_IN), 1.0, 6.0, ((0, 32),)),
        "w_mix": gaussian(arg_keys[1], (C_IN, C), C_IN ** -0.5, 0.75),
        "interp": gaussian(arg_keys[2], (16, 256), 16 ** -0.5, 1.5),
        "kernel": gaussian(arg_keys[3], (3, 3, C, C), (9 * C) ** -0.5, 0.25),
        "bias": gaussian(arg_keys[4], (C,), 0.5, 3.0, (), jnp.float32),
        "block_ids": draw_block_ids(jax.random.fold_in(arg_keys[7], 71), 0),
        "valid": draw_valid(jax.random.fold_in(arg_keys[7], 71), 0),
    }


def mix_rows(rows, w_mix):
    count = rows.shape[0]
    flat = rows.reshape(count * 16, C_IN)
    mapped = jnp.dot(flat, w_mix, preferred_element_type=jnp.float32).astype(jnp.bfloat16)
    return mapped.reshape(count, 16, C)


def reference(coarse, w_mix, interp, kernel, bias, block_ids, valid):
    mixed = mix_rows(coarse, w_mix)
    interp_f = interp.astype(jnp.float32)

    def tile_image(tile):
        picked = mixed[block_ids[tile]].astype(jnp.float32)
        fine = jnp.einsum('pkc,kf->pcf', picked, interp_f).astype(jnp.bfloat16)
        fine = fine * valid[tile][:, None, None].astype(jnp.bfloat16)
        fine = fine.reshape(PR, PC, C, 16, 16).transpose(2, 0, 3, 1, 4)
        return fine.reshape(C, TH, TW)

    tiles = lax.map(tile_image, jnp.arange(TILES, dtype=jnp.int32))
    field = tiles.reshape(N_LAT, N_LON, C, TH, TW).transpose(2, 0, 3, 1, 4).reshape(C, N_LAT * TH, N_LON * TW)
    land = valid.astype(jnp.float32).reshape(N_LAT, N_LON, PR, PC)
    land = jnp.repeat(jnp.repeat(land, 16, axis=2), 16, axis=3)
    land = land.transpose(0, 2, 1, 3).reshape(N_LAT * TH, N_LON * TW)
    padded = jnp.pad(field, ((0, 0), (1, 1), (1, 1)))
    kernel_f = kernel.astype(jnp.float32)
    width = N_LON * TW

    def band(index):
        rows = lax.dynamic_slice_in_dim(padded, (index * TH).astype(jnp.int32), TH + 2, 1).astype(jnp.float32)
        total = jnp.zeros((C, TH, width), jnp.float32)
        for tap_row in range(3):
            for tap_col in range(3):
                total = total + jnp.einsum('oc,chw->ohw', kernel_f[tap_row, tap_col], rows[:, tap_row:tap_row + TH, tap_col:tap_col + width])
        mask_rows = lax.dynamic_slice_in_dim(land, (index * TH).astype(jnp.int32), TH, 0)
        return ((total + bias[:, None, None]) * mask_rows[None]).astype(jnp.bfloat16)

    bands = lax.map(band, jnp.arange(N_LAT, dtype=jnp.int32))
    return bands.transpose(1, 0, 2, 3).reshape(C, N_LAT * TH, width)
```

```python
import functools

import jax
import jax.numpy as jnp
from jax import lax
from jax.experimental import pallas as pl
from jax.experimental.pallas import tpu as pltpu
from jax.sharding import PartitionSpec as P

PR = 18
PC = 8
SIDE = 16
STEPS = 3


def exchange(n_dev, n_lon, out_ref, in_ref, send_sem, recv_sem, own_sem):
    me = lax.axis_index("lat") * n_lon + lax.axis_index("lon")

    def copy(d):
        target = lax.rem(me + d, n_dev)
        return pltpu.make_async_remote_copy(
            src_ref=out_ref.at[target],
            dst_ref=in_ref.at[me],
            send_sem=send_sem.at[d],
            recv_sem=recv_sem.at[d],
            device_id={"lat": target // n_lon, "lon": lax.rem(target, n_lon)},
            device_id_type=pl.DeviceIdType.MESH,
        )

    own = pltpu.make_async_copy(out_ref.at[me], in_ref.at[me], own_sem)

    @pl.loop(1, n_dev)
    def _(d):
        copy(d).start()

    own.start()

    @pl.loop(1, n_dev)
    def _(d):
        copy(d).wait()

    own.wait()


def all_to_all(outgoing, n_lat, n_lon):
    n_dev = n_lat * n_lon
    return pl.pallas_call(
        functools.partial(exchange, n_dev, n_lon),
        out_shape=jax.ShapeDtypeStruct(outgoing.shape, outgoing.dtype),
        in_specs=[pl.BlockSpec(memory_space=pl.ANY)],
        out_specs=pl.BlockSpec(memory_space=pl.ANY),
        scratch_shapes=[
            pltpu.SemaphoreType.DMA((n_dev,)),
            pltpu.SemaphoreType.DMA((n_dev,)),
            pltpu.SemaphoreType.DMA,
        ],
        compiler_params=pltpu.CompilerParams(has_side_effects=True),
        name="exchange",
    )(outgoing)


NT = (((1,), (1,)), ((), ()))


def build_maps(interp, rhs, up, down):
    f32, bf16 = jnp.float32, jnp.bfloat16
    rows = SIDE * PC
    breadth = SIDE * PC
    row = lax.broadcasted_iota(jnp.int32, (rows, breadth), 0)
    lane = lax.broadcasted_iota(jnp.int32, (rows, breadth), 1)
    pick_k = lax.broadcasted_iota(jnp.int32, (rows, SIDE), 0) // PC
    pick_k = (pick_k == lax.broadcasted_iota(jnp.int32, (rows, SIDE), 1)).astype(bf16)
    repeated = jnp.dot(pick_k, interp, preferred_element_type=f32).astype(bf16)
    lane_from = lax.broadcasted_iota(jnp.int32, (SIDE, breadth), 0)
    lane_to = lax.broadcasted_iota(jnp.int32, (SIDE, breadth), 1)
    spread = (lane_from == lane_to % SIDE).astype(bf16)
    pc = row % PC
    own = [
        (lane > 0) & (pc == (lane - 1) // SIDE),
        pc == lane // SIDE,
        pc == (lane + 1) // SIDE,
    ]
    side, dy_of = pc // 4, pc % 4
    rhs[...] = jnp.zeros_like(rhs)
    up[...] = jnp.zeros_like(up)
    down[...] = jnp.zeros_like(down)

    def place(fy):
        if fy == 0:
            return SIDE // 2 - 1, breadth
        return (fy - 1) // 2, ((fy - 1) % 2) * breadth

    halo = [[None] * SIDE for _ in range(3)]
    for r in range(SIDE):
        flat = jnp.dot(repeated[:, r * SIDE:(r + 1) * SIDE], spread, preferred_element_type=f32)
        after = pltpu.roll(flat, 1, 1)
        before = pltpu.roll(flat, breadth - 1, 1)
        taps = [
            jnp.where(own[d], v, 0.0).astype(bf16) for d, v in enumerate((after, flat, before))
        ]
        edge = jnp.where((lane == 0) & (side == 0), after, 0.0)
        edge = edge + jnp.where((lane == breadth - 1) & (side == 1), before, 0.0)
        for dy in range(3):
            fy = r + 1 - dy
            part = jnp.where(dy_of == dy, edge, 0.0)
            if 0 <= fy < SIDE:
                pair, at = place(fy)
                for dx in range(3):
                    tap = (dy * 3 + dx) * rows
                    rhs[pair, tap:tap + rows, at:at + breadth] = taps[dx]
                halo[dy][fy] = part
            elif fy == SIDE:
                for dx in range(3):
                    up[dx * rows:(dx + 1) * rows, breadth:] = taps[dx]
                up[3 * rows:, breadth:] = part.astype(bf16)
            else:
                for dx in range(3):
                    down[dx * rows:(dx + 1) * rows, :breadth] = taps[dx]
                down[3 * rows:, :breadth] = part.astype(bf16)
    for fy in range(SIDE):
        pair, at = place(fy)
        total = sum(halo[dy][fy] for dy in range(3) if halo[dy][fy] is not None)
        rhs[pair, 9 * rows:, at:at + breadth] = total.astype(bf16)


def build_left(arrived, source, w_mix, kernel, grouped, left):
    f32, bf16 = jnp.float32, jnp.bfloat16
    rows = SIDE * PC
    high = PR + 2
    c_in = arrived.shape[1] // SIDE
    c_out = kernel.shape[0] // 9
    slots = lax.broadcasted_iota(jnp.int32, (source.shape[0], arrived.shape[0]), 1)
    pick = (slots == source[...]).astype(f32).astype(bf16)
    window = jnp.dot(pick, arrived[...], preferred_element_type=f32)
    grouped[...] = jnp.zeros_like(grouped)
    for k in range(SIDE):
        cell = window[:, k * c_in:(k + 1) * c_in]
        grouped[:, 0, k, :, :c_in] = cell[:high * PC].reshape(high, PC, c_in)
        grouped[:, 1, k, :, :c_in] = cell[high * PC:].reshape(high, PC, c_in)
    both = lax.dot_general(kernel[...], w_mix[...], NT, preferred_element_type=f32).astype(bf16)
    lane = lax.broadcasted_iota(jnp.int32, (c_out, rows), 1) % PC

    @pl.loop(0, high)
    def _(wr):
        cells = grouped[wr].reshape(2 * rows, 128).astype(bf16)
        res = lax.dot_general(both, cells, NT, preferred_element_type=f32)
        at = pl.ds(pl.multiple_of(wr * c_out, c_out), c_out)
        edge = jnp.zeros((c_out, rows), f32)
        for tap in range(9):
            part = res[tap * c_out:(tap + 1) * c_out]
            left[at, tap * rows:(tap + 1) * rows] = part[:, :rows].astype(bf16)
            dy, dx = divmod(tap, 3)
            if dx != 1:
                edge = jnp.where(lane == (dx // 2) * 4 + dy, part[:, rows:], edge)
        left[at, 9 * rows:] = edge.astype(bf16)


def convolve(arrived, source, w_mix, interp, kernel, bias, land, out, grouped, left, rhs, up, down, fine):
    f32 = jnp.float32
    rows = SIDE * PC
    c_out = kernel.shape[0] // 9
    step = pl.program_id(0)
    count = PR // STEPS
    many = count * c_out

    @pl.when(step == 0)
    def _():
        build_maps(interp[...], rhs, up, down)
        build_left(arrived, source, w_mix, kernel, grouped, left)

    base = pl.multiple_of(step * many, c_out)
    above = pl.ds(base, many)
    here = pl.ds(pl.multiple_of(base + c_out, c_out), many)
    below = pl.ds(pl.multiple_of(base + 2 * c_out, c_out), many)
    mask = land[step]
    pairs = SIDE // 2

    def put(total, fys):
        for half, fy in enumerate(fys):
            part = total[:, half * rows:(half + 1) * rows].reshape(count, c_out, rows)
            part = (part + bias[...][None]) * mask[:, None, :]
            fine[pl.ds(fy, many, stride=SIDE), :] = part.reshape(many, rows)

    for pair in range(pairs):
        total = jnp.dot(left[here, :], rhs[pair], preferred_element_type=f32)
        if pair == pairs - 1:
            total += jnp.dot(left[above, :3 * rows], up[:3 * rows], preferred_element_type=f32)
            total += jnp.dot(left[above, 9 * rows:], up[3 * rows:], preferred_element_type=f32)
            total += jnp.dot(left[below, 6 * rows:9 * rows], down[:3 * rows], preferred_element_type=f32)
            total += jnp.dot(left[below, 9 * rows:], down[3 * rows:], preferred_element_type=f32)
            put(total, (SIDE - 1, 0))
        else:
            put(total, (2 * pair + 1, 2 * pair + 2))
    for pr in range(count):
        block = fine[pr * c_out * SIDE:(pr + 1) * c_out * SIDE, :]
        out[:, pr * SIDE:(pr + 1) * SIDE, :] = block.reshape(c_out, SIDE, rows).astype(out.dtype)


def per_device(coarse, w_mix, interp, kernel, bias, block_ids, valid):
    n_lat = lax.axis_size("lat")
    n_lon = lax.axis_size("lon")
    n_dev = n_lat * n_lon
    lat, lon = lax.axis_index("lat"), lax.axis_index("lon")
    held = coarse.shape[0]
    channels = w_mix.shape[1]
    high, wide = PR + 2, PC + 2
    per_col = -(-wide // n_lon)
    most = -(-(-(-high // n_lat) * per_col) // 16) * 16
    i32 = jnp.int32
    first = block_ids[0, 0]
    cols = block_ids[0, n_lat * PC] - first
    spot, holder = first % held, first // held
    r0 = (spot // cols) * n_lat + holder // n_lon
    c0 = (spot % cols) * n_lon + holder % n_lon

    tile = jnp.arange(n_dev, dtype=i32)[:, None]
    place = jnp.arange(most, dtype=i32)[None, :]
    row_from = r0 + (tile // n_lon) * PR - 1
    col_from = c0 + (tile % n_lon) * PC - 1
    row = row_from + jnp.mod(lat - row_from, n_lat) + (place // per_col) * n_lat
    col = col_from + jnp.mod(lon - col_from, n_lon) + (place % per_col) * n_lon
    table = jnp.floor_divide(row, n_lat) * cols + jnp.mod(col, cols * n_lon) // n_lon
    outgoing = coarse[jnp.clip(table, 0, held - 1).reshape(-1)]
    arrived = all_to_all(outgoing.reshape(n_dev, most, coarse.shape[1]), n_lat, n_lon)

    image = valid.reshape(n_lat, n_lon, PR, PC).transpose(0, 2, 1, 3)
    image = jnp.pad(image.reshape(n_lat * PR, n_lon * PC), 1)
    live = lax.dynamic_slice(image, (lat * PR, lon * PC), (high, wide))
    wr = jnp.arange(high, dtype=i32)[:, None]
    wc = jnp.arange(wide, dtype=i32)[None, :]
    owner = jnp.mod(r0 + lat * PR - 1 + wr, n_lat) * n_lon
    owner = owner + jnp.mod(c0 + lon * PC - 1 + wc, n_lon)
    rank = (wr // n_lat) * per_col + wc // n_lon
    source = jnp.where(live > 0, owner * most + rank, -1)
    edges = jnp.repeat(source[:, ::wide - 1], 4, axis=1)
    source = jnp.concatenate([source[:, 1:-1].reshape(-1), edges.reshape(-1)])[:, None]
    land = jnp.repeat(live[1:-1, 1:-1].astype(jnp.float32), SIDE, axis=1)

    rows = SIDE * PC
    full = lambda *shape: pl.BlockSpec(shape, lambda i: (0,) * len(shape))
    arrived = arrived.reshape(n_dev * most, coarse.shape[1])
    count = PR // STEPS
    taps = kernel.reshape(9 * channels, channels)
    mixer = jnp.pad(w_mix, ((0, 128 - w_mix.shape[0]), (0, 0)))
    return pl.pallas_call(
        convolve,
        grid=(STEPS,),
        out_shape=jax.ShapeDtypeStruct((channels, PR * SIDE, rows), jnp.bfloat16),
        in_specs=[
            full(*arrived.shape), full(*source.shape), full(*mixer.shape), full(*interp.shape),
            full(*taps.shape), full(channels, 1), full(STEPS, count, rows),
        ],
        out_specs=pl.BlockSpec((channels, count * SIDE, rows), lambda i: (0, i, 0)),
        scratch_shapes=[
            pltpu.VMEM((high, 2, SIDE, PC, 128), jnp.float32),
            pltpu.VMEM((high * channels, 10 * rows), jnp.bfloat16),
            pltpu.VMEM((SIDE // 2, 10 * rows, 2 * rows), jnp.bfloat16),
            pltpu.VMEM((4 * rows, 2 * rows), jnp.bfloat16),
            pltpu.VMEM((4 * rows, 2 * rows), jnp.bfloat16),
            pltpu.VMEM((count * channels * SIDE, rows), jnp.float32),
        ],
        compiler_params=pltpu.CompilerParams(vmem_limit_bytes=60 * 1024 * 1024),
        name="convolve",
    )(arrived, source, mixer, interp, taps, bias[:, None], land.reshape(STEPS, count, rows))


def solution(mesh):
    placed = (P(("lat", "lon"), None), P(), P(), P(), P(), P(), P())
    return jax.shard_map(
        per_device, mesh=mesh, in_specs=placed, out_specs=P(None, "lat", "lon"), check_vma=False
    )
```

```python
import functools

import jax
import jax.numpy as jnp
from jax import lax
from jax.experimental import pallas as pl
from jax.experimental.pallas import tpu as pltpu
from jax.sharding import PartitionSpec as P

PR = 18
PC = 8
SIDE = 16
STEPS = 3


def exchange(n_dev, n_lon, out_ref, in_ref, send_sem, recv_sem, own_sem):
    me = lax.axis_index("lat") * n_lon + lax.axis_index("lon")

    def copy(d):
        target = lax.rem(me + d, n_dev)
        return pltpu.make_async_remote_copy(
            src_ref=out_ref.at[:, target],
            dst_ref=in_ref.at[:, me],
            send_sem=send_sem.at[d],
            recv_sem=recv_sem.at[d],
            device_id={"lat": target // n_lon, "lon": lax.rem(target, n_lon)},
            device_id_type=pl.DeviceIdType.MESH,
        )

    own = pltpu.make_async_copy(out_ref.at[:, me], in_ref.at[:, me], own_sem)

    @pl.loop(1, n_dev)
    def _(d):
        copy(d).start()

    own.start()

    @pl.loop(1, n_dev)
    def _(d):
        copy(d).wait()

    own.wait()


def all_to_all(outgoing, n_lat, n_lon):
    n_dev = n_lat * n_lon
    return pl.pallas_call(
        functools.partial(exchange, n_dev, n_lon),
        out_shape=jax.ShapeDtypeStruct(outgoing.shape, outgoing.dtype),
        in_specs=[pl.BlockSpec(memory_space=pl.ANY)],
        out_specs=pl.BlockSpec(memory_space=pl.ANY),
        scratch_shapes=[
            pltpu.SemaphoreType.DMA((n_dev,)),
            pltpu.SemaphoreType.DMA((n_dev,)),
            pltpu.SemaphoreType.DMA,
        ],
        compiler_params=pltpu.CompilerParams(has_side_effects=True),
        name="exchange",
    )(outgoing)


NT = (((1,), (1,)), ((), ()))


def offsets(ids, held, n_lat, n_lon):
    first = ids[0, 0]
    cols = ids[0, n_lat * PC] - first
    holder = lax.div(first, held)
    spot = first - holder * held
    down = lax.div(spot, cols)
    r0 = down * n_lat + lax.div(holder, n_lon)
    c0 = (spot - down * cols) * n_lon + lax.rem(holder, n_lon)
    return r0, c0, cols


def pack(n_lat, n_lon, per_col, ids, coarse, w_mix, out, cells):
    f32, bf16 = jnp.float32, jnp.bfloat16
    n_dev = n_lat * n_lon
    held, width = coarse.shape
    c_in, c_out = width // SIDE, w_mix.shape[1]
    r0, c0, cols = offsets(ids, held, n_lat, n_lon)
    lat, lon = lax.axis_index("lat"), lax.axis_index("lon")
    count = out.shape[0]
    index = lax.broadcasted_iota(jnp.int32, (count, 1), 0)
    tile, place = index % n_dev, index // n_dev
    row_from = r0 + (tile // n_lon) * PR - 1 + n_lat
    col_from = c0 + (tile % n_lon) * PC
    row = row_from + (lat - row_from) % n_lat + (place // per_col) * n_lat
    col = col_from + (lon - col_from) % n_lon + (place % per_col) * n_lon
    col = jnp.where(col >= cols * n_lon, col - cols * n_lon, col)
    table = jnp.clip((row // n_lat - 1) * cols + col // n_lon, 0, held - 1)
    pick = lax.broadcasted_iota(jnp.int32, (count, held), 1) == table
    picked = jnp.dot(pick.astype(f32).astype(bf16), coarse[...], preferred_element_type=f32)
    mixer = w_mix[...]
    for k in range(0, SIDE, 2):
        pair = [
            jnp.dot(picked[:, q * c_in:(q + 1) * c_in].astype(bf16), mixer, preferred_element_type=f32)
            for q in (k, k + 1)
        ]
        cells[:, k // 2, :] = jnp.concatenate(pair, axis=1)
    out[...] = cells[...].astype(bf16)


def build_maps(interp, rhs, up, down):
    f32, bf16 = jnp.float32, jnp.bfloat16
    rows = SIDE * PC
    breadth = SIDE * PC
    row = lax.broadcasted_iota(jnp.int32, (rows, breadth), 0)
    lane = lax.broadcasted_iota(jnp.int32, (rows, breadth), 1)
    pick_k = lax.broadcasted_iota(jnp.int32, (rows, SIDE), 0) // PC
    pick_k = (pick_k == lax.broadcasted_iota(jnp.int32, (rows, SIDE), 1)).astype(bf16)
    repeated = jnp.dot(pick_k, interp, preferred_element_type=f32).astype(bf16)
    lane_from = lax.broadcasted_iota(jnp.int32, (SIDE, breadth), 0)
    lane_to = lax.broadcasted_iota(jnp.int32, (SIDE, breadth), 1)
    spread = (lane_from == lane_to % SIDE).astype(bf16)
    pc = row % PC
    own = [
        (lane > 0) & (pc == (lane - 1) // SIDE),
        pc == lane // SIDE,
        pc == (lane + 1) // SIDE,
    ]
    side, dy_of = pc // 4, pc % 4
    rhs[...] = jnp.zeros_like(rhs)
    up[...] = jnp.zeros_like(up)
    down[...] = jnp.zeros_like(down)

    def place(fy):
        if fy == 0:
            return SIDE // 2 - 1, breadth
        return (fy - 1) // 2, ((fy - 1) % 2) * breadth

    halo = [[None] * SIDE for _ in range(3)]
    for r in range(SIDE):
        flat = jnp.dot(repeated[:, r * SIDE:(r + 1) * SIDE], spread, preferred_element_type=f32)
        after = pltpu.roll(flat, 1, 1)
        before = pltpu.roll(flat, breadth - 1, 1)
        taps = [
            jnp.where(own[d], v, 0.0).astype(bf16) for d, v in enumerate((after, flat, before))
        ]
        edge = jnp.where((lane == 0) & (side == 0), after, 0.0)
        edge = edge + jnp.where((lane == breadth - 1) & (side == 1), before, 0.0)
        for dy in range(3):
            fy = r + 1 - dy
            part = jnp.where(dy_of == dy, edge, 0.0)
            if 0 <= fy < SIDE:
                pair, at = place(fy)
                for dx in range(3):
                    tap = (dy * 3 + dx) * rows
                    rhs[pair, tap:tap + rows, at:at + breadth] = taps[dx]
                halo[dy][fy] = part
            elif fy == SIDE:
                for dx in range(3):
                    up[dx * rows:(dx + 1) * rows, breadth:] = taps[dx]
                up[3 * rows:, breadth:] = part.astype(bf16)
            else:
                for dx in range(3):
                    down[dx * rows:(dx + 1) * rows, :breadth] = taps[dx]
                down[3 * rows:, :breadth] = part.astype(bf16)
    for fy in range(SIDE):
        pair, at = place(fy)
        total = sum(halo[dy][fy] for dy in range(3) if halo[dy][fy] is not None)
        rhs[pair, 9 * rows:, at:at + breadth] = total.astype(bf16)


def build_left(n_lat, n_lon, per_col, held, ids, valid, arrived, edges, kernel, grouped, left, land, cells):
    f32, bf16 = jnp.float32, jnp.bfloat16
    n_dev = n_lat * n_lon
    rows = SIDE * PC
    high = PR + 2
    main = high * PC
    c_out = kernel.shape[0] // 9
    r0, c0, _ = offsets(ids, held, n_lat, n_lon)
    lat, lon = lax.axis_index("lat"), lax.axis_index("lon")
    index = lax.broadcasted_iota(jnp.int32, (2 * main, 1), 0)
    inner = index < main
    at = jnp.where(inner, index, index - main)
    wr = at // PC
    pc = at % PC
    side = pc // 4
    owner = (r0 + lat * PR - 1 + n_lat + wr) % n_lat * n_lon + (c0 + lon * PC + pc) % n_lon
    rank = wr // n_lat * per_col + pc // n_lon
    source = jnp.where(inner, rank * n_dev + owner, arrived.shape[0] + side * high + wr)
    tile_lat = lat + (wr == high - 1).astype(jnp.int32) - (wr == 0).astype(jnp.int32)
    tile_lon = lon + jnp.where(inner, 0, 2 * side - 1)
    slot_row = jnp.where(wr == 0, PR - 1, jnp.where(wr == high - 1, 0, wr - 1))
    slot = slot_row * PC + jnp.where(inner, pc, jnp.where(side == 0, PC - 1, 0))
    inside = (tile_lat >= 0) & (tile_lat < n_lat) & (tile_lon >= 0) & (tile_lon < n_lon)
    tile = jnp.where(inside, tile_lat * n_lon + tile_lon, -1)
    alive = (valid[...] > 0).astype(f32)
    whose = lax.broadcasted_iota(jnp.int32, (2 * main, n_dev), 1) == tile
    seen = jnp.dot(whose.astype(f32).astype(bf16), alive.astype(bf16), preferred_element_type=f32)
    spot = lax.broadcasted_iota(jnp.int32, (2 * main, PR * PC), 1) == slot
    live = jnp.sum(jnp.where(spot, seen, 0.0), axis=1, keepdims=True)
    source = jnp.where(live > 0, source, -1)

    mine = (valid[pl.ds(lat * n_lon + lon, 1), :] > 0).astype(f32)
    of_row = lax.broadcasted_iota(jnp.int32, (PR, PR * PC), 0)
    of_slot = lax.broadcasted_iota(jnp.int32, (PR, PR * PC), 1)
    by_row = jnp.where(of_slot // PC == of_row, mine, 0.0).astype(bf16)
    from_slot = lax.broadcasted_iota(jnp.int32, (PR * PC, rows), 0)
    to_lane = lax.broadcasted_iota(jnp.int32, (PR * PC, rows), 1)
    widen = (from_slot % PC == to_lane // SIDE).astype(f32).astype(bf16)
    mask = jnp.dot(by_row, widen, preferred_element_type=f32)
    for step in range(STEPS):
        land[step] = mask[step * (PR // STEPS):(step + 1) * (PR // STEPS)]

    cells[:arrived.shape[0]] = arrived[...].astype(f32)
    cells[arrived.shape[0]:] = edges[...].astype(f32)
    slots = lax.broadcasted_iota(jnp.int32, (2 * main, cells.shape[0]), 1)
    pick = (slots == source).astype(f32).astype(bf16)
    for k in range(0, SIDE, 2):
        pair = jnp.dot(pick, cells[:, k // 2, :].astype(bf16), preferred_element_type=f32)
        for q in (0, 1):
            cell = pair[:, q * c_out:(q + 1) * c_out]
            grouped[:, 0, k + q] = cell[:main].reshape(high, PC, c_out)
            grouped[:, 1, k + q] = cell[main:].reshape(high, PC, c_out)
    both = kernel[...]
    lane = lax.broadcasted_iota(jnp.int32, (c_out, rows), 1) % PC

    @pl.loop(0, high)
    def _(wr):
        cells = grouped[wr].reshape(2 * rows, c_out).astype(bf16)
        res = lax.dot_general(both, cells, NT, preferred_element_type=f32)
        at = pl.ds(pl.multiple_of(wr * c_out, c_out), c_out)
        edge = jnp.zeros((c_out, rows), f32)
        for tap in range(9):
            part = res[tap * c_out:(tap + 1) * c_out]
            left[at, tap * rows:(tap + 1) * rows] = part[:, :rows].astype(bf16)
            dy, dx = divmod(tap, 3)
            if dx != 1:
                edge = jnp.where(lane == (dx // 2) * 4 + dy, part[:, rows:], edge)
        left[at, 9 * rows:] = edge.astype(bf16)


def convolve(n_lat, n_lon, per_col, held, ids, valid, arrived, edges, interp, kernel, bias, out, grouped, left, rhs, up, down, fine, land, cells):
    f32 = jnp.float32
    rows = SIDE * PC
    c_out = kernel.shape[0] // 9
    step = pl.program_id(0)
    count = PR // STEPS
    many = count * c_out

    @pl.when(step == 0)
    def _():
        build_maps(interp[...], rhs, up, down)
        build_left(n_lat, n_lon, per_col, held, ids, valid, arrived, edges, kernel, grouped, left, land, cells)

    base = pl.multiple_of(step * many, c_out)
    above = pl.ds(base, many)
    here = pl.ds(pl.multiple_of(base + c_out, c_out), many)
    below = pl.ds(pl.multiple_of(base + 2 * c_out, c_out), many)
    mask = land[step]
    pairs = SIDE // 2

    def put(total, fys):
        for half, fy in enumerate(fys):
            part = total[:, half * rows:(half + 1) * rows].reshape(count, c_out, rows)
            part = (part + bias[...][None]) * mask[:, None, :]
            fine[pl.ds(fy, many, stride=SIDE), :] = part.reshape(many, rows)

    for pair in range(pairs):
        total = jnp.dot(left[here, :], rhs[pair], preferred_element_type=f32)
        if pair == pairs - 1:
            total += jnp.dot(left[above, :3 * rows], up[:3 * rows], preferred_element_type=f32)
            total += jnp.dot(left[above, 9 * rows:], up[3 * rows:], preferred_element_type=f32)
            total += jnp.dot(left[below, 6 * rows:9 * rows], down[:3 * rows], preferred_element_type=f32)
            total += jnp.dot(left[below, 9 * rows:], down[3 * rows:], preferred_element_type=f32)
            put(total, (SIDE - 1, 0))
        else:
            put(total, (2 * pair + 1, 2 * pair + 2))
    for pr in range(count):
        block = fine[pr * c_out * SIDE:(pr + 1) * c_out * SIDE, :]
        out[:, pr * SIDE:(pr + 1) * SIDE, :] = block.reshape(c_out, SIDE, rows).astype(out.dtype)


def per_device(coarse, w_mix, interp, kernel, bias, block_ids, valid):
    n_lat = lax.axis_size("lat")
    n_lon = lax.axis_size("lon")
    n_dev = n_lat * n_lon
    lat, lon = lax.axis_index("lat"), lax.axis_index("lon")
    held = coarse.shape[0]
    channels = w_mix.shape[1]
    high = PR + 2
    per_col = -(-PC // n_lon)
    most = -(-high // n_lat) * per_col
    count = n_dev * most
    lanes = 2 * channels
    cell = (SIDE // 2, lanes)
    i32 = jnp.int32
    vmem = pl.BlockSpec(memory_space=pltpu.VMEM)
    smem = pl.BlockSpec(memory_space=pltpu.SMEM)
    outgoing = pl.pallas_call(
        functools.partial(pack, n_lat, n_lon, per_col),
        out_shape=jax.ShapeDtypeStruct((count,) + cell, jnp.bfloat16),
        in_specs=[smem, vmem, vmem],
        out_specs=vmem,
        scratch_shapes=[pltpu.VMEM((count,) + cell, jnp.float32)],
        compiler_params=pltpu.CompilerParams(vmem_limit_bytes=40 * 1024 * 1024),
        name="pack",
    )(block_ids[:1], coarse, w_mix)
    arrived = all_to_all(outgoing.reshape((most, n_dev) + cell), n_lat, n_lon)
    arrived = arrived.reshape((count,) + cell)

    first = block_ids[0, 0] // held
    wr = jnp.arange(high, dtype=i32)[None, :]
    pc = jnp.array([[PC - 1], [0]], i32)
    owner = jnp.mod(first // n_lon + lat * PR - 1 + wr, n_lat) * n_lon
    owner = owner + jnp.mod(first % n_lon + lon * PC + pc, n_lon)
    rank = wr // n_lat * per_col + pc // n_lon
    ends = arrived[rank * n_dev + owner]
    ahead = [(i, i + 1) for i in range(n_lon - 1)]
    back = [(i + 1, i) for i in range(n_lon - 1)]
    edges = jnp.concatenate(
        [lax.ppermute(ends[0], "lon", ahead), lax.ppermute(ends[1], "lon", back)], axis=0
    )

    rows = SIDE * PC
    full = lambda *shape: pl.BlockSpec(shape, lambda i: (0,) * len(shape))
    part = PR // STEPS
    taps = kernel.reshape(9 * channels, channels)
    return pl.pallas_call(
        functools.partial(convolve, n_lat, n_lon, per_col, held),
        grid=(STEPS,),
        out_shape=jax.ShapeDtypeStruct((channels, PR * SIDE, rows), jnp.bfloat16),
        in_specs=[
            smem, full(*valid.shape), full(*arrived.shape), full(*edges.shape),
            full(*interp.shape), full(*taps.shape), full(channels, 1),
        ],
        out_specs=pl.BlockSpec((channels, part * SIDE, rows), lambda i: (0, i, 0)),
        scratch_shapes=[
            pltpu.VMEM((high, 2, SIDE, PC, channels), jnp.float32),
            pltpu.VMEM((high * channels, 10 * rows), jnp.bfloat16),
            pltpu.VMEM((SIDE // 2, 10 * rows, 2 * rows), jnp.bfloat16),
            pltpu.VMEM((4 * rows, 2 * rows), jnp.bfloat16),
            pltpu.VMEM((4 * rows, 2 * rows), jnp.bfloat16),
            pltpu.VMEM((part * channels * SIDE, rows), jnp.float32),
            pltpu.VMEM((STEPS, part, rows), jnp.float32),
            pltpu.VMEM((count + 2 * high,) + cell, jnp.float32),
        ],
        compiler_params=pltpu.CompilerParams(vmem_limit_bytes=60 * 1024 * 1024),
        name="convolve",
    )(block_ids[:1], valid, arrived, edges, interp, taps, bias[:, None])


def solution(mesh):
    placed = (P(("lat", "lon"), None), P(), P(), P(), P(), P(), P())
    return jax.shard_map(
        per_device, mesh=mesh, in_specs=placed, out_specs=P(None, "lat", "lon"), check_vma=False
    )
```

```python
import functools

import jax
import jax.numpy as jnp
from jax import lax
from jax.experimental import pallas as pl
from jax.experimental.pallas import tpu as pltpu
from jax.sharding import PartitionSpec as P

PR = 18
PC = 8
SIDE = 16
STEPS = 3


def exchange(n_dev, n_lon, out_ref, in_ref, send_sem, recv_sem, own_sem):
    me = lax.axis_index("lat") * n_lon + lax.axis_index("lon")

    def copy(d):
        target = lax.rem(me + d, n_dev)
        return pltpu.make_async_remote_copy(
            src_ref=out_ref.at[target],
            dst_ref=in_ref.at[me],
            send_sem=send_sem.at[d],
            recv_sem=recv_sem.at[d],
            device_id={"lat": target // n_lon, "lon": lax.rem(target, n_lon)},
            device_id_type=pl.DeviceIdType.MESH,
        )

    own = pltpu.make_async_copy(out_ref.at[me], in_ref.at[me], own_sem)

    @pl.loop(1, n_dev)
    def _(d):
        copy(d).start()

    own.start()

    @pl.loop(1, n_dev)
    def _(d):
        copy(d).wait()

    own.wait()


def all_to_all(outgoing, n_lat, n_lon):
    n_dev = n_lat * n_lon
    return pl.pallas_call(
        functools.partial(exchange, n_dev, n_lon),
        out_shape=jax.ShapeDtypeStruct(outgoing.shape, outgoing.dtype),
        in_specs=[pl.BlockSpec(memory_space=pltpu.VMEM)],
        out_specs=pl.BlockSpec(memory_space=pltpu.VMEM),
        scratch_shapes=[
            pltpu.SemaphoreType.DMA((n_dev,)),
            pltpu.SemaphoreType.DMA((n_dev,)),
            pltpu.SemaphoreType.DMA,
        ],
        compiler_params=pltpu.CompilerParams(has_side_effects=True),
        name="exchange",
    )(outgoing)


NT = (((1,), (1,)), ((), ()))


def offsets(ids, held, n_lat, n_lon):
    first = ids[0, 0]
    cols = ids[0, n_lat * PC] - first
    holder = lax.div(first, held)
    spot = first - holder * held
    down = lax.div(spot, cols)
    r0 = down * n_lat + lax.div(holder, n_lon)
    c0 = (spot - down * cols) * n_lon + lax.rem(holder, n_lon)
    return r0, c0, cols


def pack(n_lat, n_lon, per_col, ids, coarse, w_mix, out, cells):
    f32, bf16 = jnp.float32, jnp.bfloat16
    n_dev = n_lat * n_lon
    held, width = coarse.shape
    c_in, c_out = width // SIDE, w_mix.shape[1]
    r0, c0, cols = offsets(ids, held, n_lat, n_lon)
    lat, lon = lax.axis_index("lat"), lax.axis_index("lon")
    count = out.shape[0]
    index = lax.broadcasted_iota(jnp.int32, (count, 1), 0)
    most = count // n_dev
    passed = index >= (lax.broadcasted_iota(jnp.int32, (count, n_dev), 1) + 1) * most
    tile = jnp.sum(passed.astype(f32), axis=1, keepdims=True).astype(jnp.int32)
    place = index - tile * most
    row_from = r0 + (tile // n_lon) * PR - 1 + n_lat
    col_from = c0 + (tile % n_lon) * PC
    row = row_from + (lat - row_from) % n_lat + (place // per_col) * n_lat
    col = col_from + (lon - col_from) % n_lon + (place % per_col) * n_lon
    col = jnp.where(col >= cols * n_lon, col - cols * n_lon, col)
    table = jnp.clip((row // n_lat - 1) * cols + col // n_lon, 0, held - 1)
    pick = lax.broadcasted_iota(jnp.int32, (count, held), 1) == table
    picked = jnp.dot(pick.astype(f32).astype(bf16), coarse[...], preferred_element_type=f32)
    mixer = w_mix[...]
    for k in range(0, SIDE, 2):
        pair = [
            jnp.dot(picked[:, q * c_in:(q + 1) * c_in].astype(bf16), mixer, preferred_element_type=f32)
            for q in (k, k + 1)
        ]
        cells[:, k // 2, :] = jnp.concatenate(pair, axis=1)
    out[...] = cells[...].astype(bf16)


def build_maps(interp, rhs, up, down):
    f32, bf16 = jnp.float32, jnp.bfloat16
    rows = SIDE * PC
    breadth = SIDE * PC
    row = lax.broadcasted_iota(jnp.int32, (rows, breadth), 0)
    lane = lax.broadcasted_iota(jnp.int32, (rows, breadth), 1)
    pick_k = lax.broadcasted_iota(jnp.int32, (rows, SIDE), 0) // PC
    pick_k = (pick_k == lax.broadcasted_iota(jnp.int32, (rows, SIDE), 1)).astype(bf16)
    repeated = jnp.dot(pick_k, interp, preferred_element_type=f32).astype(bf16)
    lane_from = lax.broadcasted_iota(jnp.int32, (SIDE, breadth), 0)
    lane_to = lax.broadcasted_iota(jnp.int32, (SIDE, breadth), 1)
    spread = (lane_from == lane_to % SIDE).astype(bf16)
    pc = row % PC
    own = [
        (lane > 0) & (pc == (lane - 1) // SIDE),
        pc == lane // SIDE,
        pc == (lane + 1) // SIDE,
    ]
    side, dy_of = pc // 4, pc % 4
    rhs[...] = jnp.zeros_like(rhs)
    up[...] = jnp.zeros_like(up)
    down[...] = jnp.zeros_like(down)

    def place(fy):
        if fy == 0:
            return SIDE // 2 - 1, breadth
        return (fy - 1) // 2, ((fy - 1) % 2) * breadth

    halo = [[None] * SIDE for _ in range(3)]
    for r in range(SIDE):
        flat = jnp.dot(repeated[:, r * SIDE:(r + 1) * SIDE], spread, preferred_element_type=f32)
        after = pltpu.roll(flat, 1, 1)
        before = pltpu.roll(flat, breadth - 1, 1)
        taps = [
            jnp.where(own[d], v, 0.0).astype(bf16) for d, v in enumerate((after, flat, before))
        ]
        edge = jnp.where((lane == 0) & (side == 0), after, 0.0)
        edge = edge + jnp.where((lane == breadth - 1) & (side == 1), before, 0.0)
        for dy in range(3):
            fy = r + 1 - dy
            part = jnp.where(dy_of == dy, edge, 0.0)
            if 0 <= fy < SIDE:
                pair, at = place(fy)
                for dx in range(3):
                    tap = (dy * 3 + dx) * rows
                    rhs[pair, tap:tap + rows, at:at + breadth] = taps[dx]
                halo[dy][fy] = part
            elif fy == SIDE:
                for dx in range(3):
                    up[dx * rows:(dx + 1) * rows, breadth:] = taps[dx]
                up[3 * rows:, breadth:] = part.astype(bf16)
            else:
                for dx in range(3):
                    down[dx * rows:(dx + 1) * rows, :breadth] = taps[dx]
                down[3 * rows:, :breadth] = part.astype(bf16)
    for fy in range(SIDE):
        pair, at = place(fy)
        total = sum(halo[dy][fy] for dy in range(3) if halo[dy][fy] is not None)
        rhs[pair, 9 * rows:, at:at + breadth] = total.astype(bf16)


def choose_ends(n_lat, n_lon, per_col, held, ids, arrived, out, cells, chosen):
    f32, bf16 = jnp.float32, jnp.bfloat16
    r0, c0, _ = offsets(ids, held, n_lat, n_lon)
    lat, lon = lax.axis_index("lat"), lax.axis_index("lon")
    most = arrived.shape[0] // (n_lat * n_lon)
    count = out.shape[0]
    index = lax.broadcasted_iota(jnp.int32, (count, 1), 0)
    low = index < count // 2
    wr = jnp.where(low, index, index - count // 2)
    pc = jnp.where(low, PC - 1, 0)
    owner = (r0 + lat * PR - 1 + n_lat + wr) % n_lat * n_lon + (c0 + lon * PC + pc) % n_lon
    source = owner * most + wr // n_lat * per_col + pc // n_lon
    slots = lax.broadcasted_iota(jnp.int32, (count, arrived.shape[0]), 1)
    pick = (slots == source).astype(f32).astype(bf16)
    cells[...] = arrived[...].astype(f32)
    for j in range(SIDE // 2):
        block = cells[:, j, :].astype(bf16)
        chosen[:, j, :] = jnp.dot(pick, block, preferred_element_type=f32)
    out[...] = chosen[...].astype(bf16)


def build_left(n_lat, n_lon, per_col, held, ids, valid, arrived, edges, kernel, grouped, left, land, cells):
    f32, bf16 = jnp.float32, jnp.bfloat16
    n_dev = n_lat * n_lon
    rows = SIDE * PC
    high = PR + 2
    main = high * PC
    c_out = kernel.shape[0] // 9
    r0, c0, _ = offsets(ids, held, n_lat, n_lon)
    lat, lon = lax.axis_index("lat"), lax.axis_index("lon")
    index = lax.broadcasted_iota(jnp.int32, (2 * main, 1), 0)
    inner = index < main
    at = jnp.where(inner, index, index - main)
    wr = at // PC
    pc = at % PC
    side = pc // 4
    owner = (r0 + lat * PR - 1 + n_lat + wr) % n_lat * n_lon + (c0 + lon * PC + pc) % n_lon
    rank = wr // n_lat * per_col + pc // n_lon
    source = jnp.where(inner, owner * (arrived.shape[0] // n_dev) + rank, arrived.shape[0] + side * high + wr)
    tile_lat = lat + (wr == high - 1).astype(jnp.int32) - (wr == 0).astype(jnp.int32)
    tile_lon = lon + jnp.where(inner, 0, 2 * side - 1)
    slot_row = jnp.where(wr == 0, PR - 1, jnp.where(wr == high - 1, 0, wr - 1))
    slot = slot_row * PC + jnp.where(inner, pc, jnp.where(side == 0, PC - 1, 0))
    inside = (tile_lat >= 0) & (tile_lat < n_lat) & (tile_lon >= 0) & (tile_lon < n_lon)
    tile = jnp.where(inside, tile_lat * n_lon + tile_lon, -1)
    alive = (valid[...] > 0).astype(f32)
    whose = lax.broadcasted_iota(jnp.int32, (2 * main, n_dev), 1) == tile
    seen = jnp.dot(whose.astype(f32).astype(bf16), alive.astype(bf16), preferred_element_type=f32)
    spot = lax.broadcasted_iota(jnp.int32, (2 * main, PR * PC), 1) == slot
    live = jnp.sum(jnp.where(spot, seen, 0.0), axis=1, keepdims=True)
    source = jnp.where(live > 0, source, -1)

    mine = (valid[pl.ds(lat * n_lon + lon, 1), :] > 0).astype(f32)
    of_row = lax.broadcasted_iota(jnp.int32, (PR, PR * PC), 0)
    of_slot = lax.broadcasted_iota(jnp.int32, (PR, PR * PC), 1)
    by_row = jnp.where(of_slot // PC == of_row, mine, 0.0).astype(bf16)
    from_slot = lax.broadcasted_iota(jnp.int32, (PR * PC, rows), 0)
    to_lane = lax.broadcasted_iota(jnp.int32, (PR * PC, rows), 1)
    widen = (from_slot % PC == to_lane // SIDE).astype(f32).astype(bf16)
    mask = jnp.dot(by_row, widen, preferred_element_type=f32)
    for step in range(STEPS):
        land[step] = mask[step * (PR // STEPS):(step + 1) * (PR // STEPS)]

    cells[:arrived.shape[0]] = arrived[...].astype(f32)
    cells[arrived.shape[0]:] = edges[...].astype(f32)
    slots = lax.broadcasted_iota(jnp.int32, (2 * main, cells.shape[0]), 1)
    pick = (slots == source).astype(f32).astype(bf16)
    for k in range(0, SIDE, 2):
        pair = jnp.dot(pick, cells[:, k // 2, :].astype(bf16), preferred_element_type=f32)
        for q in (0, 1):
            cell = pair[:, q * c_out:(q + 1) * c_out]
            grouped[:, 0, k + q] = cell[:main].reshape(high, PC, c_out)
            grouped[:, 1, k + q] = cell[main:].reshape(high, PC, c_out)
    both = kernel[...]
    lane = lax.broadcasted_iota(jnp.int32, (c_out, rows), 1) % PC

    @pl.loop(0, high)
    def _(wr):
        cells = grouped[wr].reshape(2 * rows, c_out).astype(bf16)
        res = lax.dot_general(both, cells, NT, preferred_element_type=f32)
        at = pl.ds(pl.multiple_of(wr * c_out, c_out), c_out)
        edge = jnp.zeros((c_out, rows), f32)
        for tap in range(9):
            part = res[tap * c_out:(tap + 1) * c_out]
            left[at, tap * rows:(tap + 1) * rows] = part[:, :rows].astype(bf16)
            dy, dx = divmod(tap, 3)
            if dx != 1:
                edge = jnp.where(lane == (dx // 2) * 4 + dy, part[:, rows:], edge)
        left[at, 9 * rows:] = edge.astype(bf16)


def convolve(n_lat, n_lon, per_col, held, ids, valid, arrived, edges, interp, kernel, bias, out, grouped, left, rhs, up, down, fine, land, cells):
    f32 = jnp.float32
    rows = SIDE * PC
    c_out = kernel.shape[0] // 9
    step = pl.program_id(0)
    count = PR // STEPS
    many = count * c_out

    @pl.when(step == 0)
    def _():
        build_maps(interp[...], rhs, up, down)
        build_left(n_lat, n_lon, per_col, held, ids, valid, arrived, edges, kernel, grouped, left, land, cells)

    base = pl.multiple_of(step * many, c_out)
    above = pl.ds(base, many)
    here = pl.ds(pl.multiple_of(base + c_out, c_out), many)
    below = pl.ds(pl.multiple_of(base + 2 * c_out, c_out), many)
    mask = land[step]
    pairs = SIDE // 2
    diagonal = lax.broadcasted_iota(jnp.int32, (c_out, c_out), 0)
    diagonal = diagonal == lax.broadcasted_iota(jnp.int32, (c_out, c_out), 1)
    shift = jnp.sum(jnp.where(diagonal, bias[...], 0.0), axis=1, keepdims=True)

    def put(total, fys):
        for half, fy in enumerate(fys):
            part = total[:, half * rows:(half + 1) * rows].reshape(count, c_out, rows)
            part = (part + shift[None]) * mask[:, None, :]
            fine[pl.ds(fy, many, stride=SIDE), :] = part.reshape(many, rows)

    for pair in range(pairs):
        total = jnp.dot(left[here, :], rhs[pair], preferred_element_type=f32)
        if pair == pairs - 1:
            total += jnp.dot(left[above, :3 * rows], up[:3 * rows], preferred_element_type=f32)
            total += jnp.dot(left[above, 9 * rows:], up[3 * rows:], preferred_element_type=f32)
            total += jnp.dot(left[below, 6 * rows:9 * rows], down[:3 * rows], preferred_element_type=f32)
            total += jnp.dot(left[below, 9 * rows:], down[3 * rows:], preferred_element_type=f32)
            put(total, (SIDE - 1, 0))
        else:
            put(total, (2 * pair + 1, 2 * pair + 2))
    for pr in range(count):
        block = fine[pr * c_out * SIDE:(pr + 1) * c_out * SIDE, :]
        out[:, pr * SIDE:(pr + 1) * SIDE, :] = block.reshape(c_out, SIDE, rows).astype(out.dtype)


def per_device(coarse, w_mix, interp, kernel, bias, block_ids, valid):
    n_lat = lax.axis_size("lat")
    n_lon = lax.axis_size("lon")
    n_dev = n_lat * n_lon
    held = coarse.shape[0]
    channels = w_mix.shape[1]
    high = PR + 2
    per_col = -(-PC // n_lon)
    most = -(-high // n_lat) * per_col
    count = n_dev * most
    lanes = 2 * channels
    cell = (SIDE // 2, lanes)
    vmem = pl.BlockSpec(memory_space=pltpu.VMEM)
    smem = pl.BlockSpec(memory_space=pltpu.SMEM)
    outgoing = pl.pallas_call(
        functools.partial(pack, n_lat, n_lon, per_col),
        out_shape=jax.ShapeDtypeStruct((count,) + cell, jnp.bfloat16),
        in_specs=[smem, vmem, vmem],
        out_specs=vmem,
        scratch_shapes=[pltpu.VMEM((count,) + cell, jnp.float32)],
        compiler_params=pltpu.CompilerParams(vmem_limit_bytes=40 * 1024 * 1024),
        name="pack",
    )(block_ids, coarse, w_mix)
    arrived = all_to_all(outgoing.reshape((n_dev, most) + cell), n_lat, n_lon)
    arrived = arrived.reshape((count,) + cell)

    ends = pl.pallas_call(
        functools.partial(choose_ends, n_lat, n_lon, per_col, held),
        out_shape=jax.ShapeDtypeStruct((2 * high,) + cell, jnp.bfloat16),
        in_specs=[smem, vmem],
        out_specs=vmem,
        scratch_shapes=[
            pltpu.VMEM((count,) + cell, jnp.float32),
            pltpu.VMEM((2 * high,) + cell, jnp.float32),
        ],
        name="choose_ends",
    )(block_ids, arrived)
    ahead = [(i, i + 1) for i in range(n_lon - 1)]
    back = [(i + 1, i) for i in range(n_lon - 1)]
    edges = jnp.concatenate(
        [lax.ppermute(ends[:high], "lon", ahead), lax.ppermute(ends[high:], "lon", back)], axis=0
    )

    rows = SIDE * PC
    full = lambda *shape: pl.BlockSpec(shape, lambda i: (0,) * len(shape))
    part = PR // STEPS
    taps = kernel.reshape(9 * channels, channels)
    return pl.pallas_call(
        functools.partial(convolve, n_lat, n_lon, per_col, held),
        grid=(STEPS,),
        out_shape=jax.ShapeDtypeStruct((channels, PR * SIDE, rows), jnp.bfloat16),
        in_specs=[
            smem, full(*valid.shape), full(*arrived.shape), full(*edges.shape),
            full(*interp.shape), full(*taps.shape), full(1, channels),
        ],
        out_specs=pl.BlockSpec((channels, part * SIDE, rows), lambda i: (0, i, 0)),
        scratch_shapes=[
            pltpu.VMEM((high, 2, SIDE, PC, channels), jnp.float32),
            pltpu.VMEM((high * channels, 10 * rows), jnp.bfloat16),
            pltpu.VMEM((SIDE // 2, 10 * rows, 2 * rows), jnp.bfloat16),
            pltpu.VMEM((4 * rows, 2 * rows), jnp.bfloat16),
            pltpu.VMEM((4 * rows, 2 * rows), jnp.bfloat16),
            pltpu.VMEM((part * channels * SIDE, rows), jnp.float32),
            pltpu.VMEM((STEPS, part, rows), jnp.float32),
            pltpu.VMEM((count + 2 * high,) + cell, jnp.float32),
        ],
        compiler_params=pltpu.CompilerParams(vmem_limit_bytes=60 * 1024 * 1024),
        name="convolve",
    )(block_ids, valid, arrived, edges, interp, taps, bias[None, :])


def solution(mesh):
    placed = (P(("lat", "lon"), None), P(), P(), P(), P(), P(), P())
    return jax.shard_map(
        per_device, mesh=mesh, in_specs=placed, out_specs=P(None, "lat", "lon"), check_vma=False
    )
```
